32 devices in a mesh: rep: 1, fsdp: 32 (over z, y, x, core).
Axes of the slice: x: 2, y: 2, z: 4, core: 2. Of those that a mesh axis runs over, the one named last changes fastest.
Arguments:
- grads: bfloat16 [1, 24, 1280, 1280], P('rep', None, 'fsdp'), as said below
- group_counts: int32 [2], replicated, may hold values from 1 to 18, 24 in all
- owners: int32 [24], replicated, may hold values from 0 to 31, as said below
- left_stat: float32 [32, 1280, 1280], P('fsdp', 'rep'), may hold values from -4 to 4
- right_stat: float32 [32, 1280, 1280], P('fsdp', 'rep'), may hold values from -4 to 4
- left_root: bfloat16 [32, 1280, 1280], P('fsdp', 'rep'), as said below
- right_root: bfloat16 [32, 1280, 1280], P('fsdp', 'rep'), as said below
Outputs:
- left_new: float32 [32, 1280, 1280], P('fsdp', 'rep')
- right_new: float32 [32, 1280, 1280], P('fsdp', 'rep')
- update: bfloat16 [24, 1280, 1280], P(None, ('rep', 'fsdp'))
The draws below stay inside these ranges and needn't reach their ends.
Inputs may be any that keep to these rules, and one draw needn't show every extreme that they name: `grads`: block gradients of every replica group, real-valued. `owners`: no slot is named by two blocks. `group_counts`: the counts add up to 24. `left_root`: Symmetric, with a positive diagonal of about 0.5 to 2, each entry within a small symmetric perturbation of that range, and off-diagonal entries much smaller than the diagonal. `right_root`: Symmetric, with a positive diagonal of about 0.5 to 2, each entry within a small symmetric perturbation of that range, and off-diagonal entries much smaller than the diagonal.
All inputs are finite; a program needn't handle non-finite values.
Results may differ from the reference program's by a relative error of at most 0.00065.
The reference program's roundings to bfloat16 on the way count: a program that leaves them out, or rounds other values in their place, can miss the bound.
Values may be sent and summed in bfloat16 or wider, within the bound.
No kernel may reach another device: no remote copies, remote signals or barrier semaphores. Data moves between devices by JAX's collectives and lax.ppermute only.
A program may use at most 128 MiB of HBM per device.

```python
import math
import jax
import jax.numpy as jnp
import numpy as np
from jax import lax

W = 1280
REPS = 1
SLOTS = 32
NB = 24
GROUPS = 2
GROUP_MOST = 18


def draw_grads(key, part):
    keys = jax.random.split(key, 4)
    block_scale = jnp.exp(jax.random.uniform(keys[0], (1, NB, 1, 1), jnp.float32, math.log(0.5), math.log(2.0)))
    row_scale = jnp.exp(jax.random.uniform(keys[1], (1, 1, W, 1), jnp.float32, math.log(0.3), math.log(3.0)))
    column_scale = jnp.exp(jax.random.uniform(keys[2], (1, 1, 1, W), jnp.float32, math.log(0.3), math.log(3.0)))
    base = jax.random.normal(keys[3], (REPS, NB, W, W), jnp.float32)
    return (base * block_scale * row_scale * column_scale).astype(jnp.bfloat16)


def draw_owners(key, part):
    return jax.random.permutation(key, SLOTS)[:NB].astype(jnp.int32)


def root_matrix(key):
    keys = jax.random.split(key, 2)
    noise = jax.random.normal(keys[0], (SLOTS, W, W), jnp.float32)
    noise = noise * (0.5 / math.sqrt(W))
    symmetric = (noise + jnp.swapaxes(noise, 1, 2)) / math.sqrt(2.0)
    diagonal = jnp.exp(jax.random.uniform(keys[1], (SLOTS, W), jnp.float32, math.log(0.5), math.log(2.0)))
    return symmetric + diagonal[:, :, None] * jnp.eye(W, dtype=jnp.float32)[None, :, :]


def draw_left_root(key, part):
    return root_matrix(jax.random.fold_in(key, 11)).astype(jnp.bfloat16)


def draw_right_root(key, part):
    return root_matrix(jax.random.fold_in(key, 23)).astype(jnp.bfloat16)


def level_of(rng, extent, pieces, smallest, high):
    gain, own = 1.0, jax.random.fold_in(rng, 6)
    for dim, parts in pieces:
        steps = jnp.exp(jax.random.uniform(jax.random.fold_in(own, dim), (parts,), jnp.float32, smallest / len(pieces), high / len(pieces)))
        gain = gain * jnp.repeat(steps, extent[dim] // parts).reshape([-1 if axis == dim else 1 for axis in range(len(extent))])
    return gain


def split_up(count, total, reach, slope):
    weights = [(1 << 20) // math.isqrt(grade ** slope) + 1 for grade in range(2, count + 1)]
    surplus, counts = total - reach - (count - 1), [1] * (count - 1)
    while surplus > 0:
        candidates = [i for i in range(count - 1) if counts[i] < reach]
        whole, left = sum([weights[i] for i in candidates]), surplus
        for i in candidates:
            addition = min(reach - counts[i], max(1, left * weights[i] // whole), surplus)
            counts[i] = counts[i] + addition
            surplus = surplus - addition
    return np.array([reach] + counts)


def ragged_sizes(own_key, count, total, reach, skew):
    if count == 2:
        one = jax.random.randint(own_key, (), max(1, total - reach), min(reach, total - 1) + 1)
        return jnp.stack([one, total - one])
    lengths = jnp.asarray(split_up(count, total, reach, skew), jnp.int32)
    pairs = (count - 1) // 2
    donor, sink = lengths[1:1 + 2 * pairs:2], lengths[2:2 + 2 * pairs:2]
    margin = jnp.minimum(donor - 1, reach - sink)
    moved = jax.random.randint(jax.random.fold_in(own_key, 1), (pairs,), 0, 1 << 20) % (margin + 1)
    lengths = lengths.at[1:1 + 2 * pairs:2].set(donor - moved).at[2:2 + 2 * pairs:2].set(sink + moved)
    return lengths[jax.random.permutation(jax.random.fold_in(own_key, 2), count)]


def normal_values(key, extent, deviation, reach, cuts=(), kind=jnp.bfloat16):
    drawn = deviation * jax.random.normal(key, extent, jnp.float32)
    if cuts:
        drawn = drawn * level_of(key, extent, cuts, -0.22, 0.18)
    return jnp.clip(drawn, -reach, reach).astype(kind)


def setup_inputs(seed: int = 0) -> dict:
    seeds = jax.random.split(jax.random.key(seed), 8)
    grads = draw_grads(jax.random.fold_in(seeds[7], 71), 0)
    group_counts = ragged_sizes(seeds[1], GROUPS, NB, GROUP_MOST, 1).astype(jnp.int32)
    owners = draw_owners(jax.random.fold_in(seeds[7], 71), 0)
    left_stat = normal_values(seeds[3], (SLOTS, W, W), 0.5, 4.0, ((0, 32),), jnp.float32)
    right_stat = normal_values(seeds[4], (SLOTS, W, W), 0.5, 4.0, ((0, 32),), jnp.float32)
    left_root = draw_left_root(jax.random.fold_in(seeds[7], 71), 0)
    right_root = draw_right_root(jax.random.fold_in(seeds[7], 71), 0)
    return dict(grads=grads, group_counts=group_counts, owners=owners, left_stat=left_stat, right_stat=right_stat, left_root=left_root, right_root=right_root)


BETA = 0.95
EPSILON = 1e-06

def one_block(items):
    block, left_one, right_one = items
    left_gram = jnp.dot(block, block.T, preferred_element_type=jnp.float32)
    right_gram = jnp.dot(block.T, block, preferred_element_type=jnp.float32)
    halfway = jnp.dot(left_one, block, preferred_element_type=jnp.float32).astype(jnp.bfloat16)
    precond = jnp.dot(halfway, right_one, preferred_element_type=jnp.float32)
    return (left_gram, right_gram, precond)

def reference(grads, group_counts, owners, left_stat, right_stat, left_root, right_root):
    grad = lax.optimization_barrier(jnp.sum(grads.astype(jnp.float32), axis=0)).astype(jnp.bfloat16)
    width = grad.shape[1]
    coef = (1.0 - BETA) / width
    left_gram, right_gram, precond = lax.map(one_block, (grad, left_root[owners], right_root[owners]))
    left_new = BETA * left_stat + coef * jnp.zeros_like(left_stat).at[owners].set(left_gram)
    right_new = BETA * right_stat + coef * jnp.zeros_like(right_stat).at[owners].set(right_gram)
    ends = jnp.cumsum(group_counts).astype(jnp.int32)
    starts = (ends - group_counts).astype(jnp.int32)
    block_ids = jnp.arange(grad.shape[0], dtype=jnp.int32)
    member = ((block_ids[:, None] >= starts[None, :]) & (block_ids[:, None] < ends[None, :])).astype(jnp.float32)
    grad_f = grad.astype(jnp.float32)
    block_gsq = lax.optimization_barrier(jnp.sum(grad_f * grad_f, axis=(1, 2)))
    block_psq = lax.optimization_barrier(jnp.sum(precond * precond, axis=(1, 2)))
    grad_sq = lax.optimization_barrier(jnp.sum(member * block_gsq[:, None], axis=0))
    prec_sq = lax.optimization_barrier(jnp.sum(member * block_psq[:, None], axis=0))
    group_ratio = jnp.sqrt((grad_sq + EPSILON) / (prec_sq + EPSILON))
    block_ratio = lax.optimization_barrier(jnp.sum(member * group_ratio[None, :], axis=1))
    update = (precond * block_ratio[:, None, None]).astype(jnp.bfloat16)
    return (left_new, right_new, update)
```

```python
import jax
import jax.numpy as jnp
from jax import lax
from jax.experimental import pallas as pl
from jax.experimental.pallas import tpu as pltpu
from jax.sharding import PartitionSpec as P

BETA = 0.95
EPSILON = 1e-06
LANES = 128
VMEM = pl.BlockSpec(memory_space=pltpu.VMEM)
SMEM = pl.BlockSpec(memory_space=pltpu.SMEM)
ANY = pl.BlockSpec(memory_space=pl.ANY)


def side(extent, most):
    while extent % most:
        most //= 2
    return most


def pack_kernel(owners, grads, slotted, held, zeros, used, in_sems, out_sems):
    blocks, slots = grads.shape[0], slotted.shape[0]

    def load(b):
        return pltpu.make_async_copy(grads.at[b], held.at[b], in_sems.at[b])

    @pl.loop(0, blocks)
    def _(b):
        load(b).start()

    zeros[...] = jnp.zeros_like(zeros)

    @pl.loop(0, slots)
    def _(s):
        used[s] = 0

    @pl.loop(0, blocks)
    def _(b):
        used[owners[b]] = 1

    @pl.loop(0, slots)
    def _(s):
        @pl.when(used[s] == 0)
        def _():
            pltpu.make_async_copy(zeros, slotted.at[s], out_sems.at[s]).start()

    @pl.loop(0, blocks)
    def _(b):
        load(b).wait()
        s = owners[b]
        pltpu.make_async_copy(held.at[b], slotted.at[s], out_sems.at[s]).start()

    @pl.loop(0, slots)
    def _(s):
        pltpu.make_async_copy(zeros, slotted.at[s], out_sems.at[s]).wait()


def pack(owners, grads, slots):
    blocks, rows, width = grads.shape
    return pl.pallas_call(
        pack_kernel,
        out_shape=jax.ShapeDtypeStruct((slots, rows, width), grads.dtype),
        in_specs=[SMEM, ANY],
        out_specs=ANY,
        scratch_shapes=[
            pltpu.VMEM((blocks, rows, width), grads.dtype),
            pltpu.VMEM((rows, width), grads.dtype),
            pltpu.SMEM((slots,), jnp.int32),
            pltpu.SemaphoreType.DMA((blocks,)),
            pltpu.SemaphoreType.DMA((slots,)),
        ],
        cost_estimate=pl.CostEstimate(flops=0, bytes_accessed=4 * slots * rows * width, transcendentals=0),
        name="pack",
    )(owners, grads)


def unpack_kernel(owners, returned, update, sems):
    blocks = update.shape[0]

    def store(b):
        return pltpu.make_async_copy(returned.at[owners[b]], update.at[b], sems.at[b])

    @pl.loop(0, blocks)
    def _(b):
        store(b).start()

    @pl.loop(0, blocks)
    def _(b):
        store(b).wait()


def unpack(owners, returned):
    blocks = owners.shape[0]
    _, rows, width = returned.shape
    return pl.pallas_call(
        unpack_kernel,
        out_shape=jax.ShapeDtypeStruct((blocks, rows, width), returned.dtype),
        in_specs=[SMEM, VMEM],
        out_specs=ANY,
        scratch_shapes=[pltpu.SemaphoreType.DMA((blocks,))],
        cost_estimate=pl.CostEstimate(flops=0, bytes_accessed=4 * blocks * rows * width, transcendentals=0),
        name="unpack",
    )(owners, returned)


def precond_kernel(left, block, right, grad_part, mine, precond, message, halfway):
    height, width = left.shape
    step = side(width, 256)

    @pl.loop(0, width // step)
    def _(n):
        columns = pl.ds(pl.multiple_of(n * step, step), step)
        part = jnp.dot(left[...], block[:, columns], preferred_element_type=jnp.float32)
        halfway[:, columns] = part.astype(halfway.dtype)

    def body(n, total):
        columns = pl.ds(pl.multiple_of(n * step, step), step)
        part = jnp.dot(halfway[...], right[:, columns], preferred_element_type=jnp.float32)
        precond[:, columns] = part
        squares = jnp.sum((part * part).reshape(height // 8, 8, step), axis=0)
        for k in range(step // LANES):
            total = total + squares[:, k * LANES : (k + 1) * LANES]
        return total

    total = lax.fori_loop(0, width // step, body, jnp.zeros((8, LANES), jnp.float32))
    prec_part = mine[...] * jnp.sum(total, keepdims=True)
    both = jnp.concatenate([grad_part[...], prec_part], axis=0)
    message[...] = jnp.broadcast_to(both[None], message.shape)


def precondition(left, block, right, grad_part, mine, peers):
    height, width = left.shape
    return pl.pallas_call(
        precond_kernel,
        out_shape=(
            jax.ShapeDtypeStruct((height, width), jnp.float32),
            jax.ShapeDtypeStruct((peers, 2, LANES), jnp.float32),
        ),
        in_specs=[VMEM] * 5,
        out_specs=(VMEM, VMEM),
        scratch_shapes=[pltpu.VMEM((height, width), jnp.bfloat16)],
        compiler_params=pltpu.CompilerParams(vmem_limit_bytes=40 << 20),
        cost_estimate=pl.CostEstimate(
            flops=4 * height * width * width, bytes_accessed=12 * width * width, transcendentals=0
        ),
        name="precondition",
    )(left, block, right, grad_part, mine)


def graft_kernel(sums, mine, precond, scaled):
    total = jnp.sum(sums[...], axis=0)
    ratios = jnp.sqrt((total[0:1] + EPSILON) / (total[1:2] + EPSILON))
    ratio = jnp.sum(jnp.where(mine[...] > 0, ratios, 0.0), keepdims=True)
    height = precond.shape[0]
    step = side(height, 128)

    @pl.loop(0, height // step)
    def _(m):
        rows = pl.ds(pl.multiple_of(m * step, step), step)
        scaled[rows, :] = (precond[rows, :] * ratio).astype(scaled.dtype)


def graft(sums, mine, precond):
    return pl.pallas_call(
        graft_kernel,
        out_shape=jax.ShapeDtypeStruct(precond.shape, jnp.bfloat16),
        in_specs=[VMEM] * 3,
        out_specs=VMEM,
        compiler_params=pltpu.CompilerParams(vmem_limit_bytes=40 << 20),
        cost_estimate=pl.CostEstimate(flops=precond.size, bytes_accessed=6 * precond.size, transcendentals=0),
        name="graft",
    )(sums, mine, precond)


def on_device(grads, group_counts, owners, left_stat, right_stat, left_root, right_root):
    slots, reps = lax.axis_size("fsdp"), lax.axis_size("rep")
    width = left_stat.shape[2]
    half_rows = left_stat.shape[1]
    local = grads[0]
    if reps > 1:
        local = lax.psum(local.astype(jnp.float32), "rep").astype(jnp.bfloat16)
    slotted = pack(owners, local, slots)
    block = lax.all_to_all(slotted, "fsdp", split_axis=0, concat_axis=0, tiled=True)
    block = block.reshape(width, width)

    ends = jnp.cumsum(jnp.pad(group_counts, (0, LANES - group_counts.shape[0])))
    starts = ends - jnp.pad(group_counts, (0, LANES - group_counts.shape[0]))
    block_ids = jnp.arange(owners.shape[0], dtype=jnp.int32)
    member = (block_ids[:, None] >= starts[None, :]) & (block_ids[:, None] < ends[None, :])
    owned_here = owners == lax.axis_index("fsdp")
    mine = jnp.sum((member & owned_here[:, None]).astype(jnp.float32), axis=0, keepdims=True)
    local_float = local.astype(jnp.float32)
    squares = jnp.sum(local_float * local_float, axis=(1, 2))
    grad_part = jnp.sum(jnp.where(member, squares[:, None], 0.0), axis=0, keepdims=True)

    whole_root = right_root[0]
    if reps > 1:
        grad_part = grad_part / reps
        whole_root = lax.all_gather(whole_root, "rep", axis=0, tiled=True)
    precond, message = precondition(left_root[0], block, whole_root, grad_part, mine, slots)
    sums = lax.all_to_all(message, "fsdp", split_axis=0, concat_axis=0, tiled=True)
    if reps > 1:
        sums = lax.psum(sums, "rep")
    scaled = graft(sums, mine, precond).reshape(slots, half_rows // slots, width)
    returned = lax.all_to_all(scaled, "fsdp", split_axis=0, concat_axis=0, tiled=True)

    first = lax.axis_index("rep") * half_rows
    rows = lax.dynamic_slice_in_dim(block, first, half_rows, 0) if reps > 1 else block
    columns = lax.dynamic_slice_in_dim(block, first, half_rows, 1) if reps > 1 else block
    coef = (1.0 - BETA) / width
    left_gram = jnp.dot(rows, block.T, preferred_element_type=jnp.float32)
    right_gram = lax.dot_general(columns, block, (((0,), (0,)), ((), ())), preferred_element_type=jnp.float32)
    left_new = BETA * left_stat[0] + coef * left_gram
    right_new = BETA * right_stat[0] + coef * right_gram
    return (left_new[None], right_new[None], unpack(owners, returned))


def solution(mesh):
    in_specs = (
        P("rep", None, "fsdp", None),
        P(),
        P(),
        P("fsdp", "rep", None),
        P("fsdp", "rep", None),
        P("fsdp", "rep", None),
        P("fsdp", "rep", None),
    )
    out_specs = (P("fsdp", "rep", None), P("fsdp", "rep", None), P(None, ("rep", "fsdp"), None))
    return jax.shard_map(on_device, mesh=mesh, in_specs=in_specs, out_specs=out_specs, check_vma=False)
```

```python
import jax
import jax.numpy as jnp
from jax import lax
from jax.experimental import pallas as pl
from jax.experimental.pallas import tpu as pltpu
from jax.sharding import PartitionSpec as P

BETA = 0.95
EPSILON = 1e-06
LANES = 128
KERNEL_VMEM = 32 << 20
VMEM = pl.BlockSpec(memory_space=pltpu.VMEM)
SMEM = pl.BlockSpec(memory_space=pltpu.SMEM)
HBM = pl.BlockSpec(memory_space=pltpu.HBM)


def side(extent, most):
    while extent % most:
        most //= 2
    return most


def pack_kernel(owners, grads, slotted, held, zeros, used, in_sems, out_sems):
    blocks, slots = grads.shape[0], slotted.shape[0]
    loads = [pltpu.make_async_copy(grads.at[b], held.at[b], in_sems.at[b]) for b in range(blocks)]
    for load in loads:
        load.start()
    zeros[...] = jnp.zeros_like(zeros)
    for s in range(slots):
        used[s] = 0
    for b in range(blocks):
        used[owners[b]] = 1
    for s in range(slots):

        @pl.when(used[s] == 0)
        def _():
            pltpu.make_async_copy(zeros, slotted.at[s], out_sems.at[s]).start()

    for b in range(blocks):
        loads[b].wait()
        s = owners[b]
        pltpu.make_async_copy(held.at[b], slotted.at[s], out_sems.at[s]).start()
    for s in range(slots):
        pltpu.make_async_copy(zeros, slotted.at[s], out_sems.at[s]).wait()


def pack(owners, grads, slots):
    blocks, rows, width = grads.shape
    return pl.pallas_call(
        pack_kernel,
        out_shape=jax.ShapeDtypeStruct((slots, rows, width), grads.dtype),
        in_specs=[SMEM, HBM],
        out_specs=HBM,
        scratch_shapes=[
            pltpu.VMEM((blocks, rows, width), grads.dtype),
            pltpu.VMEM((rows, width), grads.dtype),
            pltpu.SMEM((slots,), jnp.int32),
            pltpu.SemaphoreType.DMA((blocks,)),
            pltpu.SemaphoreType.DMA((slots,)),
        ],
        cost_estimate=pl.CostEstimate(flops=0, bytes_accessed=4 * slots * rows * width, transcendentals=0),
        name="pack",
    )(owners, grads)


def unpack_kernel(owners, returned, update, held, in_sems, out_sems):
    blocks = update.shape[0]
    loads = [pltpu.make_async_copy(returned.at[owners[b]], held.at[b], in_sems.at[b]) for b in range(blocks)]
    stores = [pltpu.make_async_copy(held.at[b], update.at[b], out_sems.at[b]) for b in range(blocks)]
    for load in loads:
        load.start()
    for load, store in zip(loads, stores):
        load.wait()
        store.start()
    for store in stores:
        store.wait()


def unpack(owners, returned):
    blocks = owners.shape[0]
    _, rows, width = returned.shape
    return pl.pallas_call(
        unpack_kernel,
        out_shape=jax.ShapeDtypeStruct((blocks, rows, width), returned.dtype),
        in_specs=[SMEM, HBM],
        out_specs=HBM,
        scratch_shapes=[
            pltpu.VMEM((blocks, rows, width), returned.dtype),
            pltpu.SemaphoreType.DMA((blocks,)),
            pltpu.SemaphoreType.DMA((blocks,)),
        ],
        cost_estimate=pl.CostEstimate(flops=0, bytes_accessed=4 * blocks * rows * width, transcendentals=0),
        name="unpack",
    )(owners, returned)


def precond_kernel(left, block, right, grad_part, mine, precond, message, left_held, right_held, halfway, sems):
    height, width = left.shape
    lead, tile = side(height, 256), side(width, 256)
    spans = [pl.ds(0, lead), pl.ds(lead, height - lead)]
    tiles = [pl.ds(k * tile, tile) for k in range(width // tile)]
    loads = [pltpu.make_async_copy(left.at[r], left_held.at[r], sems.at[0, m]) for m, r in enumerate(spans)]
    rights = [pltpu.make_async_copy(right.at[k], right_held.at[k], sems.at[1, i]) for i, k in enumerate(tiles)]
    for copy in loads[:1] + rights + loads[1:]:
        copy.start()
    total = jnp.zeros((8, LANES), jnp.float32)
    for m, rows in enumerate(spans):
        loads[m].wait()
        for n in tiles:
            part = jnp.dot(left_held[rows, :], block[:, n], preferred_element_type=jnp.float32)
            halfway[rows, n] = part.astype(halfway.dtype)
        if m == 0:
            for copy in rights:
                copy.wait()
        for n in tiles:
            part = jnp.dot(halfway[rows, :], right_held[:, n], preferred_element_type=jnp.float32)
            precond[rows, n] = part
            squares = jnp.sum((part * part).reshape(rows.size // 8, 8, tile), axis=0)
            for k in range(tile // LANES):
                total = total + squares[:, k * LANES : (k + 1) * LANES]
    prec_part = mine[...] * jnp.sum(total, keepdims=True)
    both = jnp.concatenate([grad_part[...], prec_part], axis=0)
    message[...] = jnp.broadcast_to(both[None], message.shape)


def precondition(left, block, right, grad_part, mine, peers):
    height, width = left.shape
    left = pltpu.with_memory_space_constraint(left, pltpu.HBM)
    right = pltpu.with_memory_space_constraint(right, pltpu.HBM)
    return pl.pallas_call(
        precond_kernel,
        out_shape=(pltpu.VMEM((height, width), jnp.float32), pltpu.VMEM((peers, 2, LANES), jnp.float32)),
        in_specs=[HBM, VMEM, HBM, VMEM, VMEM],
        out_specs=(VMEM, VMEM),
        scratch_shapes=[
            pltpu.VMEM((height, width), jnp.bfloat16),
            pltpu.VMEM((width, width), jnp.bfloat16),
            pltpu.VMEM((height, width), jnp.bfloat16),
            pltpu.SemaphoreType.DMA((2, max(2, width // side(width, 256)))),
        ],
        compiler_params=pltpu.CompilerParams(vmem_limit_bytes=KERNEL_VMEM),
        cost_estimate=pl.CostEstimate(
            flops=4 * height * width * width, bytes_accessed=12 * width * width, transcendentals=0
        ),
        name="precondition",
    )(left, block, right, grad_part, mine)


def graft_kernel(sums, mine, precond, scaled):
    total = jnp.sum(sums[...], axis=0)
    ratios = jnp.sqrt((total[0:1] + EPSILON) / (total[1:2] + EPSILON))
    ratio = jnp.sum(jnp.where(mine[...] > 0, ratios, 0.0), keepdims=True)
    height = precond.shape[0]
    step = side(height, 128)

    @pl.loop(0, height // step)
    def _(m):
        rows = pl.ds(pl.multiple_of(m * step, step), step)
        scaled[rows, :] = (precond[rows, :] * ratio).astype(scaled.dtype)


def graft(sums, mine, precond):
    return pl.pallas_call(
        graft_kernel,
        out_shape=jax.ShapeDtypeStruct(precond.shape, jnp.bfloat16),
        in_specs=[VMEM, VMEM, VMEM],
        out_specs=VMEM,
        compiler_params=pltpu.CompilerParams(vmem_limit_bytes=KERNEL_VMEM),
        cost_estimate=pl.CostEstimate(flops=precond.size, bytes_accessed=6 * precond.size, transcendentals=0),
        name="graft",
    )(sums, mine, precond)


def on_device(grads, group_counts, owners, left_stat, right_stat, left_root, right_root):
    slots, reps = lax.axis_size("fsdp"), lax.axis_size("rep")
    width = left_stat.shape[2]
    half_rows = left_stat.shape[1]
    local = grads[0]
    if reps > 1:
        local = lax.psum(local.astype(jnp.float32), "rep").astype(jnp.bfloat16)
    slotted = pack(owners, local, slots)
    block = lax.all_to_all(slotted, "fsdp", split_axis=0, concat_axis=0, tiled=True)
    block = block.reshape(width, width)

    ends = jnp.cumsum(jnp.pad(group_counts, (0, LANES - group_counts.shape[0])))
    starts = ends - jnp.pad(group_counts, (0, LANES - group_counts.shape[0]))
    block_ids = jnp.arange(owners.shape[0], dtype=jnp.int32)
    member = (block_ids[:, None] >= starts[None, :]) & (block_ids[:, None] < ends[None, :])
    owned_here = owners == lax.axis_index("fsdp")
    mine = jnp.sum((member & owned_here[:, None]).astype(jnp.float32), axis=0, keepdims=True)
    local_float = local.astype(jnp.float32)
    squares = jnp.sum(local_float * local_float, axis=(1, 2))
    grad_part = jnp.sum(jnp.where(member, squares[:, None], 0.0), axis=0, keepdims=True)

    whole_root = right_root[0]
    if reps > 1:
        grad_part = grad_part / reps
        whole_root = lax.all_gather(whole_root, "rep", axis=0, tiled=True)
    precond, message = precondition(left_root[0], block, whole_root, grad_part, mine, slots)
    sums = lax.all_to_all(message, "fsdp", split_axis=0, concat_axis=0, tiled=True)
    if reps > 1:
        sums = lax.psum(sums, "rep")
    scaled = graft(sums, mine, precond).reshape(slots, half_rows // slots, width)
    returned = lax.all_to_all(scaled, "fsdp", split_axis=0, concat_axis=0, tiled=True)

    first = lax.axis_index("rep") * half_rows
    rows = lax.dynamic_slice_in_dim(block, first, half_rows, 0) if reps > 1 else block
    columns = lax.dynamic_slice_in_dim(block, first, half_rows, 1) if reps > 1 else block
    coef = (1.0 - BETA) / width
    left_gram = jnp.dot(rows, block.T, preferred_element_type=jnp.float32)
    right_gram = lax.dot_general(columns, block, (((0,), (0,)), ((), ())), preferred_element_type=jnp.float32)
    left_new = BETA * left_stat[0] + coef * left_gram
    right_new = BETA * right_stat[0] + coef * right_gram
    return (left_new[None], right_new[None], unpack(owners, returned))


def solution(mesh):
    in_specs = (
        P("rep", None, "fsdp", None),
        P(),
        P(),
        P("fsdp", "rep", None),
        P("fsdp", "rep", None),
        P("fsdp", "rep", None),
        P("fsdp", "rep", None),
    )
    out_specs = (P("fsdp", "rep", None), P("fsdp", "rep", None), P(None, ("rep", "fsdp"), None))
    return jax.shard_map(on_device, mesh=mesh, in_specs=in_specs, out_specs=out_specs, check_vma=False)
```

```python
import jax
import jax.numpy as jnp
from jax import lax
from jax.experimental import pallas as pl
from jax.experimental.pallas import tpu as pltpu
from jax.sharding import PartitionSpec as P

BETA = 0.95
EPSILON = 1e-06
LANES = 128
KERNEL_VMEM = 32 << 20
VMEM = pl.BlockSpec(memory_space=pltpu.VMEM)
SMEM = pl.BlockSpec(memory_space=pltpu.SMEM)
HBM = pl.BlockSpec(memory_space=pltpu.HBM)


def side(extent, most):
    while extent % most:
        most //= 2
    return most


def pack_kernel(owners_far, grads, slotted, held, zeros, owners, used, owner_sem, in_sems, out_sems):
    blocks, slots = grads.shape[0], slotted.shape[0]
    loads = [pltpu.make_async_copy(grads.at[b], held.at[b], in_sems.at[b]) for b in range(blocks)]
    load_owners = pltpu.make_async_copy(owners_far, owners, owner_sem)
    load_owners.start()
    for load in loads:
        load.start()
    zeros[...] = jnp.zeros_like(zeros)
    for s in range(slots):
        used[s] = 0
    load_owners.wait()
    for b in range(blocks):
        used[owners[b]] = 1
    for s in range(slots):

        @pl.when(used[s] == 0)
        def _():
            pltpu.make_async_copy(zeros, slotted.at[s], out_sems.at[s]).start()

    for b in range(blocks):
        loads[b].wait()
        s = owners[b]
        pltpu.make_async_copy(held.at[b], slotted.at[s], out_sems.at[s]).start()
    for s in range(slots):
        pltpu.make_async_copy(zeros, slotted.at[s], out_sems.at[s]).wait()


def pack(owners, grads, slots):
    blocks, rows, width = grads.shape
    return pl.pallas_call(
        pack_kernel,
        out_shape=jax.ShapeDtypeStruct((slots, rows, width), grads.dtype),
        in_specs=[HBM, HBM],
        out_specs=HBM,
        scratch_shapes=[
            pltpu.VMEM((blocks, rows, width), grads.dtype),
            pltpu.VMEM((rows, width), grads.dtype),
            pltpu.SMEM((blocks,), jnp.int32),
            pltpu.SMEM((slots,), jnp.int32),
            pltpu.SemaphoreType.DMA,
            pltpu.SemaphoreType.DMA((blocks,)),
            pltpu.SemaphoreType.DMA((slots,)),
        ],
        cost_estimate=pl.CostEstimate(flops=0, bytes_accessed=4 * slots * rows * width, transcendentals=0),
        name="pack",
    )(pltpu.with_memory_space_constraint(owners, pltpu.HBM), grads)


def unpack_kernel(owners, returned, update, sems):
    blocks = update.shape[0]
    stores = [pltpu.make_async_copy(returned.at[owners[b]], update.at[b], sems.at[b]) for b in range(blocks)]
    for store in stores:
        store.start()
    for store in stores:
        store.wait()


def unpack(owners, returned):
    blocks = owners.shape[0]
    _, rows, width = returned.shape
    return pl.pallas_call(
        unpack_kernel,
        out_shape=jax.ShapeDtypeStruct((blocks, rows, width), returned.dtype),
        in_specs=[SMEM, VMEM],
        out_specs=HBM,
        scratch_shapes=[pltpu.SemaphoreType.DMA((blocks,))],
        compiler_params=pltpu.CompilerParams(vmem_limit_bytes=KERNEL_VMEM),
        cost_estimate=pl.CostEstimate(flops=0, bytes_accessed=4 * blocks * rows * width, transcendentals=0),
        name="unpack",
    )(owners, returned)


def precond_kernel(
    left, block, right, grad_part, mine, precond, message, kept, left_held, right_held, halfway, sems
):
    height, width = left.shape
    lead, tile = side(height, 256), side(width, 256)
    spans = [pl.ds(0, lead), pl.ds(lead, height - lead)]
    tiles = [pl.ds(k * tile, tile) for k in range(width // tile)]
    loads = [pltpu.make_async_copy(left.at[r], left_held.at[r], sems.at[0, m]) for m, r in enumerate(spans)]
    rights = [pltpu.make_async_copy(right.at[k], right_held.at[k], sems.at[1, i]) for i, k in enumerate(tiles)]
    keep = pltpu.make_async_copy(block, kept, sems.at[0, len(spans)])
    for copy in loads[:1] + rights + loads[1:]:
        copy.start()
    total = jnp.zeros((8, LANES), jnp.float32)
    for m, rows in enumerate(spans):
        loads[m].wait()
        for n in tiles:
            part = jnp.dot(left_held[rows, :], block[:, n], preferred_element_type=jnp.float32)
            halfway[rows, n] = part.astype(halfway.dtype)
        if m == 0:
            for copy in rights:
                copy.wait()
            keep.start()
        for n in tiles:
            part = jnp.dot(halfway[rows, :], right_held[:, n], preferred_element_type=jnp.float32)
            precond[rows, n] = part
            squares = jnp.sum((part * part).reshape(rows.size // 8, 8, tile), axis=0)
            for k in range(tile // LANES):
                total = total + squares[:, k * LANES : (k + 1) * LANES]
    prec_part = mine[...] * jnp.sum(total, keepdims=True)
    both = jnp.concatenate([grad_part[...], prec_part], axis=0)
    message[...] = jnp.broadcast_to(both[None], message.shape)
    keep.wait()


def precondition(left, block, right, grad_part, mine, peers):
    height, width = left.shape
    left = pltpu.with_memory_space_constraint(left, pltpu.HBM)
    right = pltpu.with_memory_space_constraint(right, pltpu.HBM)
    return pl.pallas_call(
        precond_kernel,
        out_shape=(
            pltpu.VMEM((height, width), jnp.float32),
            pltpu.VMEM((peers, 2, LANES), jnp.float32),
            pltpu.HBM(block.shape, block.dtype),
        ),
        in_specs=[HBM, VMEM, HBM, VMEM, VMEM],
        out_specs=(VMEM, VMEM, HBM),
        scratch_shapes=[
            pltpu.VMEM((height, width), jnp.bfloat16),
            pltpu.VMEM((width, width), jnp.bfloat16),
            pltpu.VMEM((height, width), jnp.bfloat16),
            pltpu.SemaphoreType.DMA((2, max(3, width // side(width, 256)))),
        ],
        compiler_params=pltpu.CompilerParams(vmem_limit_bytes=KERNEL_VMEM),
        cost_estimate=pl.CostEstimate(
            flops=4 * height * width * width, bytes_accessed=12 * width * width, transcendentals=0
        ),
        name="precondition",
    )(left, block, right, grad_part, mine)


def graft_kernel(sums, mine, precond, scaled, out, sems):
    total = jnp.sum(sums[...], axis=0)
    ratios = jnp.sqrt((total[0:1] + EPSILON) / (total[1:2] + EPSILON))
    ratio = jnp.sum(jnp.where(mine[...] > 0, ratios, 0.0), keepdims=True)
    height = precond.shape[0]
    step = side(height, 128)
    spans = [pl.ds(m, step) for m in range(0, height, step)]
    stores = [pltpu.make_async_copy(out.at[r], scaled.at[r], sems.at[i]) for i, r in enumerate(spans)]
    for rows, store in zip(spans, stores):
        out[rows, :] = (precond[rows, :] * ratio).astype(out.dtype)
        store.start()
    for store in stores:
        store.wait()


def graft(sums, mine, precond):
    height = precond.shape[0]
    return pl.pallas_call(
        graft_kernel,
        out_shape=pltpu.HBM(precond.shape, jnp.bfloat16),
        in_specs=[VMEM, VMEM, VMEM],
        out_specs=HBM,
        scratch_shapes=[
            pltpu.VMEM(precond.shape, jnp.bfloat16),
            pltpu.SemaphoreType.DMA((height // side(height, 128),)),
        ],
        compiler_params=pltpu.CompilerParams(vmem_limit_bytes=KERNEL_VMEM),
        cost_estimate=pl.CostEstimate(flops=precond.size, bytes_accessed=6 * precond.size, transcendentals=0),
        name="graft",
    )(sums, mine, precond)


def on_device(grads, group_counts, owners, left_stat, right_stat, left_root, right_root):
    slots, reps = lax.axis_size("fsdp"), lax.axis_size("rep")
    width = left_stat.shape[2]
    half_rows = left_stat.shape[1]
    local = grads[0]
    if reps > 1:
        local = lax.psum(local.astype(jnp.float32), "rep").astype(jnp.bfloat16)
    slotted = pack(owners, local, slots)
    block = lax.all_to_all(slotted, "fsdp", split_axis=0, concat_axis=0, tiled=True)
    block = block.reshape(width, width)

    ends = jnp.cumsum(jnp.pad(group_counts, (0, LANES - group_counts.shape[0])))
    starts = ends - jnp.pad(group_counts, (0, LANES - group_counts.shape[0]))
    block_ids = jnp.arange(owners.shape[0], dtype=jnp.int32)
    member = (block_ids[:, None] >= starts[None, :]) & (block_ids[:, None] < ends[None, :])
    owned_here = owners == lax.axis_index("fsdp")
    mine = jnp.sum((member & owned_here[:, None]).astype(jnp.float32), axis=0, keepdims=True)
    local_float = local.astype(jnp.float32)
    squares = jnp.sum(local_float * local_float, axis=(1, 2))
    grad_part = jnp.sum(jnp.where(member, squares[:, None], 0.0), axis=0, keepdims=True)

    whole_root = right_root[0]
    if reps > 1:
        grad_part = grad_part / reps
        whole_root = lax.all_gather(whole_root, "rep", axis=0, tiled=True)
    precond, message, block = precondition(left_root[0], block, whole_root, grad_part, mine, slots)
    sums = lax.all_to_all(message, "fsdp", split_axis=0, concat_axis=0, tiled=True)
    if reps > 1:
        sums = lax.psum(sums, "rep")
    scaled = graft(sums, mine, precond).reshape(slots, half_rows // slots, width)
    returned = lax.all_to_all(scaled, "fsdp", split_axis=0, concat_axis=0, tiled=True)

    first = lax.axis_index("rep") * half_rows
    rows = lax.dynamic_slice_in_dim(block, first, half_rows, 0) if reps > 1 else block
    columns = lax.dynamic_slice_in_dim(block, first, half_rows, 1) if reps > 1 else block
    coef = (1.0 - BETA) / width
    left_gram = jnp.dot(rows, block.T, preferred_element_type=jnp.float32)
    right_gram = lax.dot_general(columns, block, (((0,), (0,)), ((), ())), preferred_element_type=jnp.float32)
    left_new = BETA * left_stat[0] + coef * left_gram
    right_new = BETA * right_stat[0] + coef * right_gram
    return (left_new[None], right_new[None], unpack(owners, returned))


def solution(mesh):
    in_specs = (
        P("rep", None, "fsdp", None),
        P(),
        P(),
        P("fsdp", "rep", None),
        P("fsdp", "rep", None),
        P("fsdp", "rep", None),
        P("fsdp", "rep", None),
    )
    out_specs = (P("fsdp", "rep", None), P("fsdp", "rep", None), P(None, ("rep", "fsdp"), None))
    return jax.shard_map(on_device, mesh=mesh, in_specs=in_specs, out_specs=out_specs, check_vma=False)
```
